128 devices in a mesh: replica: 4 (over x), data: 32 (over z, y, core).
Axes of the slice: x: 4, y: 4, z: 4, core: 2. Of those that a mesh axis runs over, the one named last changes fastest.
Arguments:
- img_x: bfloat16 [32768, 1024], P(('replica', 'data'))
- txt_x: bfloat16 [32768, 1024], P(('replica', 'data'))
- w_img: bfloat16 [1024, 1024], replicated
- w_txt: bfloat16 [1024, 1024], replicated
- log_temp: float32 [1], replicated
- logit_bias: float32 [1], replicated
Outputs:
- output 1: float32 [1], replicated
- output 2: float32 [1], replicated
- output 3: float32 [1], replicated
- output 4: float32 [1024, 1024], replicated
- output 5: float32 [1024, 1024], replicated
All inputs are finite; a program needn't handle non-finite values.
Results may differ from the reference program's by a relative error of at most 0.001.
Values are sent between devices in bfloat16 or wider.
A program may use at most 1 GiB of HBM per device.

```python
import math
import jax
import jax.numpy as jnp
from jax import lax

LOCAL_BATCH = 256
NUM_DEVICES = 128
IMG_FEAT = 1024
TXT_FEAT = 1024
EMBED_DIM = 1024
LATENT_RANK = 8

GLOBAL_BATCH = LOCAL_BATCH * NUM_DEVICES


def setup_inputs(seed: int = 0) -> dict:
    key_list = jax.random.split(jax.random.key(seed), 12)
    latent = jax.random.normal(key_list[0], (NUM_DEVICES, LOCAL_BATCH, LATENT_RANK), jnp.float32)
    dev_mean = jax.random.normal(key_list[1], (NUM_DEVICES, 1, LATENT_RANK), jnp.float32)
    latent = (latent + 0.8 * dev_mean).reshape(GLOBAL_BATCH, LATENT_RANK)
    mix_img = jax.random.normal(key_list[2], (LATENT_RANK, IMG_FEAT), jnp.float32) * LATENT_RANK ** -0.5
    mix_txt = jax.random.normal(key_list[3], (LATENT_RANK, TXT_FEAT), jnp.float32) * LATENT_RANK ** -0.5
    shared = jax.random.normal(key_list[4], (LATENT_RANK, EMBED_DIM), jnp.float32)
    img_x = 0.7 * (jnp.dot(latent, mix_img) + jax.random.normal(key_list[5], (GLOBAL_BATCH, IMG_FEAT), jnp.float32))
    txt_x = 0.7 * (jnp.dot(latent, mix_txt) + jax.random.normal(key_list[6], (GLOBAL_BATCH, TXT_FEAT), jnp.float32))
    w_img = jnp.dot(mix_img.T, shared) * (LATENT_RANK ** 0.5 / IMG_FEAT) + jax.random.normal(key_list[7], (IMG_FEAT, EMBED_DIM), jnp.float32) * IMG_FEAT ** -0.5
    w_txt = jnp.dot(mix_txt.T, shared) * (LATENT_RANK ** 0.5 / TXT_FEAT) + jax.random.normal(key_list[8], (TXT_FEAT, EMBED_DIM), jnp.float32) * TXT_FEAT ** -0.5
    log_temp = math.log(4.0) + jax.random.uniform(key_list[9], (1,), jnp.float32, -0.3, 0.3)
    logit_bias = -math.log(GLOBAL_BATCH) + jax.random.uniform(key_list[10], (1,), jnp.float32, -0.5, 0.5)
    return {"img_x": img_x.astype(jnp.bfloat16), "txt_x": txt_x.astype(jnp.bfloat16), "w_img": w_img.astype(jnp.bfloat16), "w_txt": w_txt.astype(jnp.bfloat16), "log_temp": log_temp.astype(jnp.float32), "logit_bias": logit_bias.astype(jnp.float32)}


def normalize(raw):
    return raw * lax.rsqrt(jnp.sum(raw * raw, axis=-1, keepdims=True))


def reference(img_x, txt_x, w_img, w_txt, log_temp, logit_bias):
    img_raw = jnp.dot(img_x, w_img, preferred_element_type=jnp.float32)
    txt_raw = jnp.dot(txt_x, w_txt, preferred_element_type=jnp.float32)
    img_unit, img_pull = jax.vjp(normalize, img_raw)
    txt_unit, txt_pull = jax.vjp(normalize, txt_raw)
    img_emb = img_unit.astype(jnp.bfloat16)
    txt_emb = txt_unit.astype(jnp.bfloat16)
    temp_scale = jnp.exp(log_temp[0])
    bias_val = logit_bias[0]
    col_ids = jnp.arange(GLOBAL_BATCH)[None, :]
    row_ids = jnp.arange(LOCAL_BATCH)[:, None]

    def block_step(state_in, block_in):
        d_txt_acc, loss_acc, temp_acc, bias_acc = state_in
        img_blk, blk_idx = block_in
        sim_tile = jnp.dot(img_blk, txt_emb.T, preferred_element_type=jnp.float32)
        logits = temp_scale * sim_tile + bias_val
        labels = jnp.where(col_ids == row_ids + blk_idx * LOCAL_BATCH, 1.0, -1.0)
        loss_part = -jnp.sum(jax.nn.log_sigmoid(labels * logits))
        grad_tile = -labels * jax.nn.sigmoid(-labels * logits) / GLOBAL_BATCH
        grad_b = grad_tile.astype(jnp.bfloat16)
        d_img_blk = temp_scale * jnp.dot(grad_b, txt_emb, preferred_element_type=jnp.float32)
        d_txt_acc = d_txt_acc + jnp.dot(grad_b.T, img_blk, preferred_element_type=jnp.float32)
        new_state = (d_txt_acc, loss_acc + loss_part, temp_acc + jnp.sum(grad_tile * sim_tile), bias_acc + jnp.sum(grad_tile))
        return new_state, d_img_blk

    init_state = (jnp.zeros((GLOBAL_BATCH, EMBED_DIM), jnp.float32), jnp.zeros((), jnp.float32), jnp.zeros((), jnp.float32), jnp.zeros((), jnp.float32))
    img_blocks = img_emb.reshape(NUM_DEVICES, LOCAL_BATCH, EMBED_DIM)
    final_state, d_img_blocks = lax.scan(block_step, init_state, (img_blocks, jnp.arange(NUM_DEVICES)))
    d_txt_acc, loss_sum, temp_sum, bias_sum = final_state
    d_img = d_img_blocks.reshape(GLOBAL_BATCH, EMBED_DIM)
    d_txt = temp_scale * d_txt_acc
    d_img_raw = img_pull(d_img)[0].astype(jnp.bfloat16)
    d_txt_raw = txt_pull(d_txt)[0].astype(jnp.bfloat16)
    d_w_img = jnp.dot(img_x.T, d_img_raw, preferred_element_type=jnp.float32)
    d_w_txt = jnp.dot(txt_x.T, d_txt_raw, preferred_element_type=jnp.float32)
    loss_out = jnp.reshape(loss_sum / GLOBAL_BATCH, (1,))
    d_log_temp = jnp.reshape(temp_scale * temp_sum, (1,))
    d_logit_bias = jnp.reshape(bias_sum, (1,))
    return (loss_out, d_log_temp, d_logit_bias, d_w_img, d_w_txt)
```

```python
import functools

import jax
import jax.numpy as jnp
from jax import lax
from jax.experimental import pallas as pl
from jax.experimental.pallas import tpu as pltpu
from jax.sharding import PartitionSpec as P

LOG2E = 1.4426950408889634
LN2 = 0.6931471805599453
MESH = pl.DeviceIdType.MESH
VMEM_BYTES = 67043328
F32 = jnp.float32
BF16 = jnp.bfloat16
NN = (((1,), (0,)), ((), ()))
NT = (((1,), (1,)), ((), ()))
TN = (((0,), (0,)), ((), ()))
BOTH = range(2)
DIMS = range(3)


def digits(word):
    return tuple(int(c, 36) for c in word)


def dot(a, b, dims):
    return lax.dot_general(a, b, dims, preferred_element_type=F32)


def position():
    d = lax.axis_index("data")
    chip = [lax.axis_index("replica"), lax.rem(lax.div(d, 2), 4), lax.div(d, 8)]
    return chip, lax.rem(d, 2)


def device(chip, core):
    return (chip[0], (chip[2] * 4 + chip[1]) * 2 + core)


def partner(v, kind):
    t = v + kind
    return lax.rem(t + 5 - 2 * lax.rem(t, 2) - kind, 4)


def neighbour(chip, core, dim, kind):
    return device([partner(v, kind) if i == dim else v for i, v in enumerate(chip)], core)


def copy_to(src, dst, send, recv, dev):
    return pltpu.make_async_remote_copy(src, dst, send, recv, device_id=dev, device_id_type=MESH)


def parts_of(h):
    a = h // 24 * 8 if h % 24 == 0 else (h // 3 + 7) // 8 * 8
    b = (h - a) // 16 * 8
    return [(0, a), (a, b), (a + b, h - a - b)]


EARLY = digits("0124")
LATE = digits("356")


def score_kernel(rows, width, sc, x_img, x_txt, w_img, w_txt, du_img, du_txt, sums,
                 raw, xb, ie, te, g, sbuf, rbuf, tmp, far, near, s0, s1, fin, acc,
                 load_sem, ag_send, ag_recv, tx_send, tx_recv, rs_send, rs_recv, dt_send, dt_recv, credit):
    h = rows // 2
    parts = parts_of(h)
    chip, core = position()
    other = device(chip, 1 - core)
    nbr = [[neighbour(chip, core, dim, kind) for dim in DIMS] for kind in BOTH]

    loads = []
    for i, (src, dst) in enumerate(((x_img, xb.at[0]), (x_txt, xb.at[1]),
                                    (w_img, sbuf.at[0, 0:width]), (w_txt, sbuf.at[1, 0:width]))):
        loads.append(pltpu.make_async_copy(src, dst, load_sem.at[i]))
        loads[-1].start()
    barrier = pltpu.get_barrier_semaphore()
    for dev in (*nbr[0], *nbr[1], other):
        pl.semaphore_signal(barrier, inc=1, device_id=dev, device_id_type=MESH)

    def irow(s, hh):
        if s in EARLY:
            return hh * 4 * h + EARLY.index(s) * h
        return (8 + hh * 3 + LATE.index(s)) * h if s in LATE else (14 + hh) * h

    def trow(s, hh, c=0):
        if s in EARLY:
            return (hh * 8 + c * 4 + EARLY.index(s)) * h
        return (16 + hh * 6 + c * 3 + LATE.index(s)) * h if s in LATE else (28 + c * 2 + hh) * h

    emb = (ie, te)
    row = (irow, trow)

    for kind in BOTH:
        loads[kind].wait()
        loads[2 + kind].wait()
        step = min(256, width)

        def project(j, _, kind=kind):
            cols = pl.ds(pl.multiple_of(j * step, step), step)
            raw[kind, :, cols] = dot(xb[kind], sbuf[kind, 0:width, cols], NN)
            return 0

        lax.fori_loop(0, width // step, project, 0)
        for hh in BOTH:
            u = raw[kind, hh * h:(hh + 1) * h, :]
            unit = u * lax.rsqrt(jnp.sum(u * u, axis=1, keepdims=True))
            emb[kind][row[kind](0, hh):row[kind](0, hh) + h, :] = unit.astype(BF16)

    ways = [digits(w) for w in "0023 0146 0215 1045 1113 1226".split()]
    whole = (0, h)
    ag = [(dim, (0, hh), (1 << dim, hh), whole) for hh in BOTH for dim in DIMS]
    ag += [(dim, (s, hh), (t, hh), whole) for hh, dim, s, t in ways]
    ag += [(dim, (7 ^ (1 << dim), hh), (7, hh), parts[dim]) for hh in BOTH for dim in DIMS]

    def ag_copy(kind, m):
        dim, (s, hs), (t, ht), (at, n) = ag[m]
        src = row[kind](s, hs) + at
        dst = row[kind](t, ht) + at
        return copy_to(emb[kind].at[src:src + n], emb[kind].at[dst:dst + n],
                       ag_send.at[kind, m], ag_recv.at[kind, m], nbr[kind][dim])

    def ag_start(k):
        for dim in DIMS:
            for kind in BOTH:
                ag_copy(kind, k * 3 + dim).start()

    def ag_wait(*ks):
        for k in ks:
            for dim in DIMS:
                for kind in BOTH:
                    ag_copy(kind, k * 3 + dim).wait_recv()

    share = [digits(w) for w in "014 81c 135 93d g3j m3p s2u".split()]

    def tx_copy(i):
        src, n, dst = (v * h for v in share[i])
        return copy_to(te.at[src:src + n], te.at[dst:dst + n], tx_send.at[i], tx_recv.at[i], other)

    k1, k0 = sc[0], sc[1]
    acc[:] = jnp.zeros_like(acc)

    def fold(x):
        return jnp.sum(x.reshape(x.shape[0] // 8, 8, x.shape[1]), axis=0)

    def entries(s, r0, c0, diagonal=False):
        tm, tn = s.shape
        z = s * k1 + k0
        if diagonal:
            i = lax.broadcasted_iota(jnp.int32, (tm, tn), 0)
            j = lax.broadcasted_iota(jnp.int32, (tm, tn), 1)
            eye = (i == j) & (i < h)
            z = jnp.where(eye, -z, z)
        low = jnp.minimum(z, 0.0)
        high = z - low
        w = jnp.exp2(low - high)
        p = jnp.exp2(low) * (1.0 / (1.0 + w))
        if diagonal:
            p = jnp.where(eye, -p, p)
        acc[0, :, 0:tn] += fold(high)
        acc[1, :, 0:tn] += fold(p)
        acc[2, :, 0:tn] += fold(p * s)
        ws = [w[8 * i:8 * i + 8] for i in range(tm // 8)]
        while len(ws) > 1:
            odd = ws[-1:] if len(ws) % 2 else []
            ws = [ws[i] + (ws[i + 1] + ws[i] * ws[i + 1]) for i in range(0, len(ws) - 1, 2)] + odd
        x = ws[0]
        u = 1.0 + x
        acc[3, :, 0:tn] += jnp.log(u) + jnp.where(x < 1.0, x - (u - 1.0), 0.0) / u
        g[pl.ds(r0, tm), pl.ds(c0, tn)] = p.astype(BF16)

    def score(r0, c0, tm, tn):
        return dot(ie[pl.ds(r0, tm), :], te[pl.ds(c0, tn), :], NT)

    def tile(r0, c0, tm, tn, diagonal=False):
        entries(score(r0, c0, tm, tn), r0, c0, diagonal)

    def tiles(n, tm, tn, at, first=0):
        a, b = s0.at[0:tm, 0:tn], s1.at[0:tm, 0:tn]

        def place(t):
            r, c = at(t)
            return pl.multiple_of(r, h), pl.multiple_of(c, h)

        def scores(t, dst):
            dst[:] = score(*place(t), tm, tn)

        scores(first, a)

        def pair(i, _):
            t = first + 2 * i
            scores(t + 1, b)
            entries(a[:], *place(t))
            scores(jnp.minimum(t + 2, first + n - 1), a)
            entries(b[:], *place(t + 1))
            return 0

        lax.fori_loop(0, n // 2, pair, 0)

    pl.semaphore_wait(barrier, 7)
    ag_start(0)
    tx_copy(0).start()
    ag_start(1)
    tx_copy(1).start()

    ag_wait(0)
    ag_start(2)
    tx_copy(2).start()
    tile(0, 0, 4 * h, 4 * h, True)
    tx_copy(0).wait_recv()
    tx_copy(2).wait_recv()
    tile(0, 4 * h, 4 * h, 4 * h)

    ag_wait(1)
    ag_start(3)
    tx_copy(3).start()
    tile(4 * h, 8 * h, 4 * h, 4 * h, True)
    tx_copy(1).wait_recv()
    tx_copy(3).wait_recv()
    tile(4 * h, 12 * h, 4 * h, 4 * h)
    tiles(4, 4 * h, 4 * h, lambda t: (t // 2 * 4 * h, (1 - t // 2) * 8 * h + t % 2 * 4 * h))

    ag_wait(2)
    ag_start(4)
    tx_copy(4).start()
    tx_copy(4).wait_recv()
    tiles(6, 4 * h, 2 * h, lambda t: (t % 2 * 4 * h, 16 * h + t // 2 * 2 * h))

    ag_wait(3)
    ag_start(5)
    tx_copy(5).start()
    tiles(8, 6 * h, 2 * h, lambda t: (8 * h, t * 2 * h))
    ag_wait(4, 5)
    tx_copy(6).start()
    tx_copy(5).wait_recv()
    tiles(6, 6 * h, 2 * h, lambda t: (8 * h, t * 2 * h), 8)
    tiles(6, 4 * h, 2 * h, lambda t: (t % 2 * 4 * h, 22 * h + t // 2 * 2 * h))
    tx_copy(6).wait_recv()
    tiles(4, 7 * h, 2 * h, lambda t: (t % 2 * 7 * h, 28 * h + t // 2 * 2 * h))
    tiles(8, 2 * h, 4 * h, lambda t: (14 * h, t * 4 * h))

    near_of = {1: 0, 2: 1, 4: 2}

    def rs_copy(kind, m, dim, src, dst, n):
        return copy_to(sbuf.at[kind, src:src + n], rbuf.at[kind, dst:dst + n],
                       rs_send.at[kind, m], rs_recv.at[kind, m], nbr[kind][dim])

    def r1(s, hh):
        return (2 + near_of[s] * 2 + hh) * h

    rs = [(dim, irow(7, hh) + parts[dim][0], hh * h + parts[dim][0], parts[dim][1]) for hh in BOTH for dim in DIMS]
    rs += [(dim, irow(t, hh), r1(s, hh), h) for hh, dim, s, t in ways]
    rs += [(dim, irow(1 << dim, hh), (8 + dim * 2 + hh) * h, h) for hh in BOTH for dim in DIMS]

    def rs_do(kind, lo, hi, what):
        for m in range(lo, hi):
            getattr(rs_copy(kind, m, *rs[m]), what)()

    groups = [(*digits("esu"), [(7, 0), (7, 1)], digits("06"), None)]
    groups += [(*digits(w), [(s, hh) for s in LATE], digits(v[:2]), digits(v[2:]))
               for hh, w, v in ((0, "8gj", "6903"), (1, "bmp", "9c36"))]
    groups += [(*digits(w), [(s, hh) for s in EARLY], digits(v[:2]), digits(v[2:]))
               for hh, w, v in ((0, "004", "cf69"), (1, "48c", "fi9c"))]
    nstep = min(256, width)

    def settle(kind, blocks, sends, needs, add=None):
        if needs is not None:
            rs_do(kind, *needs, "wait_recv")
        for i, (s, hh) in enumerate(blocks):
            at = irow(s, hh)

            def total(lo, n, extra, i=i):
                v = tmp[i * h + lo:i * h + lo + n, :]
                if add is not None:
                    v = v + add[i * h + lo:i * h + lo + n, :]
                if extra is not None:
                    v = v + rbuf[kind, extra:extra + n, :].astype(F32)
                return v

            if s == 0:
                fin[kind, hh * h:(hh + 1) * h, :] = total(0, h, None)
            elif s in near_of:
                sbuf[kind, at:at + h, :] = total(0, h, r1(s, hh)).astype(BF16)
            elif s == 7:
                sbuf[kind, at:at + h, :] = total(0, h, None).astype(BF16)
            else:
                with_extra = {6: 0, 5: 1, 3: 2}[s]
                for k, (lo, n) in enumerate(parts):
                    extra = hh * h + lo if k == with_extra else None
                    sbuf[kind, at + lo:at + lo + n, :] = total(lo, n, extra).astype(BF16)
        rs_do(kind, *sends, "start")

    def dt_copy(i, n):
        return copy_to(far.at[0:n], near.at[0:n], dt_send.at[i], dt_recv.at[i], other)

    for q, (ri, own, par, blocks, sends, needs) in enumerate(groups):
        n = len(blocks) * h
        if q > 0:
            pl.semaphore_wait(credit.at[q - 1], 1)
            dt_copy(q - 1, len(groups[q - 1][3]) * h).wait_send()

        def d_txt(j, dst, c0, n=n):
            cols = pl.ds(pl.multiple_of(j * nstep, nstep), nstep)
            dst[0:n, cols] = dot(g[:, c0 * h:c0 * h + n], ie[:, cols], TN)

        def d_img(j, n=n, ri=ri):
            cols = pl.ds(pl.multiple_of(j * nstep, nstep), nstep)
            tmp[0:n, cols] = dot(g[ri * h:ri * h + n, :], te[:, cols], NN)

        def loop(f):
            lax.fori_loop(0, width // nstep, lambda j, _: (f(j), 0)[1], 0)

        loop(functools.partial(d_txt, dst=far, c0=par))
        dt_copy(q, n).start()
        loop(d_img)
        settle(0, blocks, sends, needs)
        loop(functools.partial(d_txt, dst=tmp, c0=own))
        dt_copy(q, n).wait_recv()
        settle(1, blocks, sends, needs, near)
        if q + 1 < len(groups):
            pl.semaphore_signal(credit.at[q], inc=1, device_id=other, device_id_type=MESH)

    sums[:] = jnp.zeros_like(sums)
    loss = LN2 * acc[0] + acc[3]
    for i, v in enumerate((loss, acc[2], acc[1])):
        v = jnp.sum(v, axis=0, keepdims=True)
        total = v[:, 0:128]
        for j in range(1, v.shape[1] // 128):
            total = total + v[:, j * 128:(j + 1) * 128]
        sums[i:i + 1, :] = total

    for kind, out in ((0, du_img), (1, du_txt)):
        for hh in BOTH:
            for dim in DIMS:
                m = 12 + hh * 3 + dim
                rs_copy(kind, m, *rs[m]).wait_recv()
            d = fin[kind, hh * h:(hh + 1) * h, :]
            for dim in DIMS:
                at = (8 + dim * 2 + hh) * h
                d = d + rbuf[kind, at:at + h, :].astype(F32)
            d = d * sc[2]
            u = raw[kind, hh * h:(hh + 1) * h, :]
            r = lax.rsqrt(jnp.sum(u * u, axis=1, keepdims=True))
            u = u * r
            along = jnp.sum(d * u, axis=1, keepdims=True)
            out[hh * h:(hh + 1) * h, :] = (r * (d - u * along)).astype(BF16)

    for kind in BOTH:
        for m in range(len(ag)):
            ag_copy(kind, m).wait_send()
        rs_do(kind, 0, len(rs), "wait_send")
    for i in range(len(share)):
        tx_copy(i).wait_send()
    dt_copy(len(groups) - 1, len(groups[-1][3]) * h).wait_send()


def scores_and_grads(sc, img_x, txt_x, w_img, w_txt):
    rows, width = img_x.shape
    h = rows // 2
    any_spec = pl.BlockSpec(memory_space=pl.ANY)
    vmem = pl.BlockSpec(memory_space=pltpu.VMEM)
    dma = pltpu.SemaphoreType.DMA
    copies = dma((2, 18))
    group = pltpu.VMEM((4 * h, width), F32)
    square = pltpu.VMEM((7 * h, 4 * h), F32)

    def block(n, w=width):
        return pltpu.VMEM((n * h, w), BF16)

    def both(*shape, dtype=BF16):
        return pltpu.VMEM((2, *shape), dtype)

    return pl.pallas_call(
        functools.partial(score_kernel, rows, width),
        out_shape=(jax.ShapeDtypeStruct((rows, width), BF16), jax.ShapeDtypeStruct((rows, width), BF16),
                   jax.ShapeDtypeStruct((8, 128), F32)),
        in_specs=[pl.BlockSpec(memory_space=pltpu.SMEM)] + [any_spec] * 4,
        out_specs=(vmem, vmem, vmem),
        scratch_shapes=[
            both(rows, width, dtype=F32), both(rows, width), block(16), block(32), block(16, 32 * h),
            both(16 * h, width), both(14 * h, width),
            group, group, group, square, square, both(rows, width, dtype=F32),
            pltpu.VMEM((4, 8, 4 * h), F32),
            dma((4,)), copies, copies, dma((7,)), dma((7,)), copies, copies,
            dma((5,)), dma((5,)), pltpu.SemaphoreType.REGULAR((4,)),
        ],
        compiler_params=pltpu.CompilerParams(collective_id=0, has_side_effects=True,
                                             vmem_limit_bytes=VMEM_BYTES),
        name="scores",
    )(sc, img_x, txt_x, w_img, w_txt)


def colours_of(width):
    n = width // 128
    a = -(-n // 3)
    b = -(-(n - a) // 2)
    return [(0, a * 128), (a * 128, b * 128), ((a + b) * 128, (n - a - b) * 128)]


def weight_kernel(rows, width, x_img, x_txt, du_img, du_txt, part, dw_img, dw_txt, total,
                  xm, um, mine, theirs, r1, r2, sbuf, sr,
                  load_sem, load_send, load_recv, s_send, s_recv, a_send, a_recv, b_send, b_recv,
                  c_send, c_recv, d_send, d_recv, e_send, e_recv, out_sem, free_sem):
    chip, core = position()
    other = device(chip, 1 - core)
    kinds = (core, 1 - core)
    nbr = [[neighbour(chip, core, dim, k) for dim in DIMS] for k in kinds]
    top = [lax.div(lax.rem(c + 1 - core, 4), 2) for c in chip]
    low = [lax.rem(c + 1 - core, 2) for c in chip]
    colours = colours_of(width)
    big = width // 8
    small = width // 64

    def pick(bits, s):
        return sum((lax.rem(b + (s >> i & 1), 2) << i for i, b in enumerate(bits)), 0)

    barrier = pltpu.get_barrier_semaphore()
    for dev in (*nbr[0], *nbr[1], other):
        pl.semaphore_signal(barrier, inc=1, device_id=dev, device_id_type=MESH)

    x_refs, du_refs = (x_img, x_txt), (du_img, du_txt)

    def for_core(f):
        for c in BOTH:
            @pl.when(core == c)
            def _(c=c):
                f(c)

    def own_loads(c):
        return (pltpu.make_async_copy(x_refs[c], xm.at[0:rows], load_sem.at[0]),
                pltpu.make_async_copy(du_refs[c], um.at[0:rows], load_sem.at[1]))

    def give(c):
        return (copy_to(x_refs[1 - c], xm.at[rows:2 * rows], load_send.at[0], load_recv.at[0], other),
                copy_to(du_refs[1 - c], um.at[rows:2 * rows], load_send.at[1], load_recv.at[1], other))

    sbuf[0] = part[:]
    for_core(lambda c: [cp.start() for cp in own_loads(c)])
    pl.semaphore_wait(barrier, 7)
    for_core(lambda c: [cp.start() for cp in give(c)])

    def scalar_copy(i):
        dev = other if i == 0 else nbr[(i - 1) // 3][(i - 1) % 3]
        return copy_to(sbuf.at[i], sr.at[i], s_send.at[i], s_recv.at[i], dev)

    def scalar_step(i):
        scalar_copy(i).wait_recv()
        sbuf[i + 1] = sbuf[i] + sr[i]

    scalar_copy(0).start()
    for cp in own_loads(0):
        cp.wait()
    for cp in give(0):
        cp.wait_recv()

    step = min(256, width)

    def weights(j, _):
        cols = pl.ds(pl.multiple_of(j * step, step), step)
        v = dot(xm[:], um[:, cols], TN)
        mine[:, :, cols] = v.reshape(8, big, step)
        return 0

    lax.fori_loop(0, width // step, weights, 0)
    scalar_step(0)

    def scatter_plan():
        plan = []
        for stage in DIMS:
            for c in DIMS:
                dims = [c, (c + 1) % 3, (c + 2) % 3]
                d = dims[2 - stage]
                gone = sum(1 << e for e in dims[3 - stage:])
                for s in range(8):
                    if s >> d & 1 and not s & gone:
                        plan.append((stage, c, d, s))
        return plan

    plan = scatter_plan()

    def slots(stage, c):
        return [(i, p) for i, p in enumerate(plan) if p[0] == stage and p[1] == c]

    home = pick(top, 0)

    def view(level, s, c):
        lo, n = colours[c]
        if level == 0:
            return mine.at[pick(top, s), :, lo:lo + n]
        return mine.at[home, pl.ds(pl.multiple_of(pick(low, s) * small, small), small), lo:lo + n]

    def landing(level, i, c):
        lo, n = colours[c]
        r = r1 if level == 0 else r2
        return r.at[[k for k, p in enumerate(plan) if p[1] == c].index(i), :, lo:lo + n]

    def scatter_copy(level, i):
        stage, c, d, s = plan[i]
        sems = (a_send, a_recv) if level == 0 else (b_send, b_recv)
        return copy_to(view(level, s, c), landing(level, i, c), sems[0].at[i], sems[1].at[i], nbr[level][d])

    def gather_copy(level, i):
        stage, c, d, s = plan[i]
        sems = (d_send, d_recv) if level == 0 else (c_send, c_recv)
        ref = view(level, s ^ (1 << d), c)
        return copy_to(ref, ref, sems[0].at[i], sems[1].at[i], nbr[level][d])

    def gather_arrival(level, i):
        stage, c, d, s = plan[i]
        sems = (d_send, d_recv) if level == 0 else (c_send, c_recv)
        ref = view(level, s, c)
        return copy_to(ref, ref, sems[0].at[i], sems[1].at[i], nbr[level][d])

    for level in BOTH:
        for stage in DIMS:
            k = 1 + level * 3 + stage
            scalar_copy(k).start()
            for c in DIMS:
                for i, _ in slots(stage, c):
                    scatter_copy(level, i).start()
            for c in DIMS:
                for i, (_, _, d, s) in slots(stage, c):
                    scatter_copy(level, i).wait_recv()
                    v = view(level, s ^ (1 << d), c)
                    v[:] = v[:] + landing(level, i, c)[:]
            scalar_step(k)
            for c in DIMS:
                for i, _ in slots(stage, c):
                    scatter_copy(level, i).wait_send()
        for dev in nbr[level]:
            pl.semaphore_signal(free_sem.at[level], inc=1, device_id=dev, device_id_type=MESH)
    total[:] = sbuf[7]

    def hand_copy(i, s, c):
        lo, n = colours[c]
        b = pick(top, s)
        return copy_to(mine.at[b, :, lo:lo + n], theirs.at[b, :, lo:lo + n], e_send.at[i], e_recv.at[i], other)

    pl.semaphore_wait(free_sem.at[1], 3)
    for stage in (2, 1, 0):
        for c in DIMS:
            for i, _ in slots(stage, c):
                gather_copy(1, i).start()
        for c in DIMS:
            for i, _ in slots(stage, c):
                gather_arrival(1, i).wait_recv()
    hands = []
    pl.semaphore_wait(free_sem.at[0], 3)
    for stage in (2, 1, 0):
        for c in DIMS:
            for i, _ in slots(stage, c):
                gather_copy(0, i).start()
        if stage == 2:
            for c in DIMS:
                hands.append((len(hands), 0, c))
                hand_copy(*hands[-1]).start()
        for c in DIMS:
            for i, (_, _, d, s) in slots(stage, c):
                gather_arrival(0, i).wait_recv()
                hands.append((len(hands), s, c))
                hand_copy(*hands[-1]).start()

    def outs(c):
        refs = (dw_img, dw_txt)
        return (pltpu.make_async_copy(mine, refs[c], out_sem.at[0]),
                pltpu.make_async_copy(theirs, refs[1 - c], out_sem.at[1]))

    for_core(lambda c: outs(c)[0].start())
    for hand in hands:
        hand_copy(*hand).wait_recv()
    for_core(lambda c: outs(c)[1].start())
    for cp in outs(0):
        cp.wait()
    for cp in give(0):
        cp.wait_send()
    for i in range(7):
        scalar_copy(i).wait_send()
    for level in BOTH:
        for i in range(len(plan)):
            gather_copy(level, i).wait_send()
    for hand in hands:
        hand_copy(*hand).wait_send()


def weight_grads(img_x, txt_x, du_img, du_txt, part):
    rows, width = img_x.shape
    any_spec = pl.BlockSpec(memory_space=pl.ANY)
    vmem = pl.BlockSpec(memory_space=pltpu.VMEM)
    dma = pltpu.SemaphoreType.DMA
    two = dma((2,))
    shape = (8, width // 8, width)
    pair = pltpu.VMEM((2 * rows, width), BF16)
    whole = pltpu.VMEM(shape, F32)
    dw_img, dw_txt, total = pl.pallas_call(
        functools.partial(weight_kernel, rows, width),
        out_shape=(jax.ShapeDtypeStruct(shape, F32), jax.ShapeDtypeStruct(shape, F32),
                   jax.ShapeDtypeStruct((8, 128), F32)),
        in_specs=[any_spec] * 4 + [vmem],
        out_specs=(any_spec, any_spec, vmem),
        scratch_shapes=[
            pair, pair, whole, whole,
            pltpu.VMEM((7, width // 8, width), F32),
            pltpu.VMEM((7, width // 64, width), F32),
            pltpu.VMEM((8, 8, 128), F32),
            pltpu.VMEM((7, 8, 128), F32),
            two, two, two, dma((7,)), dma((7,)), *[dma((21,))] * 8, dma((24,)), dma((24,)), two,
            pltpu.SemaphoreType.REGULAR((2,)),
        ],
        compiler_params=pltpu.CompilerParams(collective_id=1, has_side_effects=True, vmem_limit_bytes=VMEM_BYTES),
        name="weights",
    )(img_x, txt_x, du_img, du_txt, part)
    return dw_img.reshape(width, width), dw_txt.reshape(width, width), total


def solution(mesh):
    devices = mesh.shape["replica"] * mesh.shape["data"]
    batch = ("replica", "data")

    def local_fn(img_x, txt_x, w_img, w_txt, log_temp, logit_bias):
        total_rows = img_x.shape[0] * devices
        temp = jnp.exp(log_temp[0])
        sc = jnp.stack([temp * LOG2E, logit_bias[0] * LOG2E, temp / total_rows])
        du_img, du_txt, part = scores_and_grads(sc, img_x, txt_x, w_img, w_txt)
        dw_img, dw_txt, total = weight_grads(img_x, txt_x, du_img, du_txt, part)
        sums = jnp.sum(total, axis=1) / total_rows
        return sums[0:1], temp * sums[1:2], sums[2:3], dw_img, dw_txt

    spec = P(batch, None)
    return jax.shard_map(local_fn, mesh=mesh, in_specs=(spec, spec, P(), P(), P(), P()),
                         out_specs=(P(), P(), P(), P(), P()), check_vma=False)
```
